32 devices in a mesh: dp: 4 (over x, y), tp: 8 (over z, core).
Axes of the slice: x: 2, y: 2, z: 4, core: 2. Of those that a mesh axis runs over, the one named last changes fastest.
Arguments:
- x: bfloat16 [8192, 4096], P('dp'), parts along dimension 0
- gain: bfloat16 [4096], replicated
- wq: bfloat16 [4096, 12288], P(None, 'tp')
- wk: bfloat16 [4096, 1024], P(None, 'tp')
- wv: bfloat16 [4096, 1024], P(None, 'tp')
- wo: bfloat16 [12288, 4096], P('tp')
Outputs:
- output: bfloat16 [8192, 4096], P('dp'), parts along dimension 0
There are 4 independent parts. The reference program is written for one: setup_inputs(seed, part) draws one part's arguments, and reference() takes and returns one part's arrays. A program takes and returns all parts, laid end to end along the dimension named above; an argument that names none is the same for every part.
All inputs are finite; a program needn't handle non-finite values.
Results may differ from the reference program's by a relative error of at most 0.012.
Values are sent between devices in bfloat16 or wider.
A program may use at most 2 GiB of HBM per device.

```python
import jax
import jax.numpy as jnp
from jax import lax

ROWS = 2048
D = 4096
HEADS = 96
KV_HEADS = 8
HEAD = 128
THETA = 10000


def setup_inputs(seed: int = 0, part: int = 0) -> dict:
    kx, kn, kq, kk, kv, ko = jax.random.split(jax.random.key(seed), 6)

    def weights(key, rows, columns):
        return jax.random.normal(key, (rows, columns), jnp.float32) * rows**-0.5

    drawn = {
        "x": jax.random.normal(jax.random.fold_in(kx, part), (ROWS, D), jnp.float32),
        "gain": 1 + 0.1 * jax.random.normal(kn, (D,), jnp.float32),
        "wq": 2 * weights(kq, D, HEADS * HEAD),
        "wk": 2 * weights(kk, D, KV_HEADS * HEAD),
        "wv": 4 * weights(kv, D, KV_HEADS * HEAD),
        "wo": weights(ko, HEADS * HEAD, D),
    }
    return {k: v.astype(jnp.bfloat16) for k, v in drawn.items()}


def normed(x, gain):
    wide = x.astype(jnp.float32)
    scale = lax.rsqrt(jnp.mean(wide * wide, -1, keepdims=True) + 1e-6)
    return (wide * scale * gain.astype(jnp.float32)).astype(jnp.bfloat16)


def turned(t, place, theta):
    half = t.shape[-1] // 2
    angle = place.astype(jnp.float32)[:, None] * theta ** (-jnp.arange(half, dtype=jnp.float32) / half)
    cos, sin = jnp.cos(angle)[:, None], jnp.sin(angle)[:, None]
    a, b = t[..., :half].astype(jnp.float32), t[..., half:].astype(jnp.float32)
    return jnp.concatenate([a * cos - b * sin, b * cos + a * sin], -1).astype(jnp.bfloat16)


def matmul(a, w):
    return jnp.dot(a, w, preferred_element_type=jnp.float32).astype(jnp.bfloat16)


def einsum(form, a, b):
    return jnp.einsum(form, a.astype(jnp.float32), b.astype(jnp.float32))


def attention(q, k, v):
    scores = einsum("tgsd,ugd->gstu", q, k) * q.shape[-1] ** -0.5
    token = jnp.arange(q.shape[0])
    scores = jnp.where(token[:, None] >= token, scores, -jnp.inf)
    weights = jax.nn.softmax(scores, -1).astype(jnp.bfloat16)
    return einsum("gstu,ugd->tgsd", weights, v).astype(jnp.bfloat16)


def reference(x, gain, wq, wk, wv, wo):
    a, place = normed(x, gain), jnp.arange(ROWS)
    q = turned(matmul(a, wq).reshape(ROWS, HEADS, HEAD), place, THETA).reshape(ROWS, KV_HEADS, -1, HEAD)
    k = turned(matmul(a, wk).reshape(ROWS, KV_HEADS, HEAD), place, THETA)
    v = matmul(a, wv).reshape(ROWS, KV_HEADS, HEAD)
    seen = attention(q, k, v).reshape(ROWS, HEADS * HEAD)
    return (x.astype(jnp.float32) + jnp.dot(seen, wo, preferred_element_type=jnp.float32)).astype(jnp.bfloat16)
```

```python
import functools

import jax
import jax.numpy as jnp
import numpy as np
from jax import lax
from jax.experimental import pallas as pl
from jax.experimental.pallas import tpu as pltpu
from jax.sharding import PartitionSpec as P

HEAD = 128
THETA = 10000
NEG = -1e30
HIDDEN = 2 * NEG
LOG2E = 1.4426950408889634
MESH = pl.DeviceIdType.MESH
F32, BF16 = jnp.float32, jnp.bfloat16


def _dot(a, b, ca=1, cb=0):
    return lax.dot_general(a, b, (((ca,), (cb,)), ((), ())), preferred_element_type=F32)


class Sizes:
    def __init__(self, rows, d, heads, chunk=256, sub=32, slots=8, hop=2, piece=3):
        self.rows, self.d, self.heads = rows, d, heads
        self.chunk, self.sub, self.slots, self.hop, self.piece = chunk, sub, slots, hop, piece
        self.chunks = rows // chunk
        self.per = chunk // sub
        self.ns = rows // sub
        self.half = d // 2
        self.os = d // 8


def _kernel(z, x_hbm, gain_ref, cs_ref, wq_hbm, wk_hbm, wv_hbm, wo_hbm, y_hbm,
            wq_s, wkv_s, wo_s, x_s, a_s, q_s, k_s, vt_s, seen_s, top_s, mix_s,
            own_s, give_s, got_s, part_s, out_s,
            w_sem, x_sem, give_sem, got_sem, part_sem, out_sem, fin_sem, fwd_sem, pair_sem, slot_free, got_free):
    CH, SUB, K, D, PER, NS, NCH = z.chunk, z.sub, z.slots, z.hop, z.per, z.ns, z.chunks
    half = z.half
    me = lax.axis_index("tp")
    core, line = lax.rem(me, 2), lax.div(me, 2)
    mate = me + 1 - 2 * core
    place = jnp.where(core == 0, line, 3 - line)

    def at(q):
        return {"tp": jnp.where(core == 0, 2 * q, 7 - 2 * q)}

    to_mate = {"tp": mate}
    mine = pl.multiple_of(core * half, half)
    theirs = pl.multiple_of((1 - core) * half, half)
    own_cols, mate_cols = pl.ds(mine, half), pl.ds(theirs, half)
    pairs = z.heads // 2
    barrier = pltpu.get_barrier_semaphore()
    for other in range(1, 8):
        pl.semaphore_signal(barrier, inc=1, device_id={"tp": lax.rem(me + other, 8)}, device_id_type=MESH)

    def x_copy(i):
        return pltpu.make_async_copy(x_hbm.at[pl.ds(i * CH, CH), :], x_s.at[lax.rem(i, 2)], x_sem.at[lax.rem(i, 2)])

    def wq_copy(j):
        return pltpu.make_async_copy(wq_hbm.at[:, pl.ds(j * 2 * HEAD, 2 * HEAD)], wq_s.at[j], w_sem.at[j])

    wk_copy = pltpu.make_async_copy(wk_hbm, wkv_s.at[:, pl.ds(0, HEAD)], w_sem.at[pairs])
    wv_copy = pltpu.make_async_copy(wv_hbm, wkv_s.at[:, pl.ds(HEAD, HEAD)], w_sem.at[pairs + 1])

    def wo_copy(j):
        return pltpu.make_async_copy(wo_hbm.at[:, pl.ds(j * z.os, z.os)], wo_s.at[j], w_sem.at[pairs + 2 + j])

    x_copy(0).start()
    wk_copy.start()
    wv_copy.start()
    for j in range(pairs):
        wq_copy(j).start()
    vt_s[HEAD:, :] = jnp.ones((8, z.rows), BF16)
    pl.semaphore_wait(barrier, 7)

    def give_copy(i):
        b = lax.rem(i, 2)
        return pltpu.make_async_remote_copy(give_s.at[b], got_s.at[b], give_sem.at[b], got_sem.at[b], device_id=to_mate, device_id_type=MESH)

    def part_copy(s, lane, q):
        k = lax.rem(s, K)
        return pltpu.make_async_remote_copy(out_s.at[k], part_s.at[lane, k], out_sem.at[0, k], part_sem.at[lane, k], device_id=at(q), device_id_type=MESH)

    def piece_of_y(s, cols):
        return y_hbm.at[pl.ds(s * SUB, SUB), cols]

    def fin_copy(s, n, q):
        k = lax.rem(s, K)
        return pltpu.make_async_remote_copy(out_s.at[k], piece_of_y(s, own_cols), out_sem.at[n, k], fin_sem.at[s], device_id=at(q), device_id_type=MESH)

    def fin_pair_copy(s):
        k = lax.rem(s, K)
        return pltpu.make_async_remote_copy(out_s.at[k], piece_of_y(s, own_cols), out_sem.at[2, k], pair_sem.at[s], device_id=to_mate, device_id_type=MESH)

    def fin_here(s):
        k = lax.rem(s, K)
        return pltpu.make_async_copy(out_s.at[k], piece_of_y(s, own_cols), out_sem.at[3, k])

    def fwd_pair_copy(s):
        return pltpu.make_async_remote_copy(piece_of_y(s, own_cols), piece_of_y(s, own_cols), fwd_sem.at[0, s], pair_sem.at[s], device_id=to_mate, device_id_type=MESH)

    def fwd_line_copy(s):
        return pltpu.make_async_remote_copy(piece_of_y(s, own_cols), piece_of_y(s, own_cols), fwd_sem.at[1, s], fin_sem.at[s], device_id=at(3), device_id_type=MESH)

    def owner_sends(s):
        return fin_copy(s, 0, 0), fin_copy(s, 1, 2), fin_pair_copy(s), fin_here(s)

    def free_slot(lane, q):
        pl.semaphore_signal(slot_free.at[lane], inc=1, device_id=at(q), device_id_type=MESH)

    lead = jnp.where(place == 2, D, jnp.where(place == 1, 2 * D, 0))
    late = jnp.where(place == 3, 4 * D, 3 * D)

    def combine(s):
        b, r, k = lax.rem(lax.div(s, PER), 2), lax.rem(s, PER), lax.rem(s, K)
        rows = pl.ds(pl.multiple_of(r * SUB, SUB), SUB)

        @pl.when(r == 0)
        def _():
            give_copy(lax.div(s, PER)).wait_recv()

        def base():
            return own_s[b, rows, :] + got_s[b, rows, :].astype(F32)

        @pl.when((place == 3) | (place == 0))
        def _():
            @pl.when(s >= K)
            def _():
                part_copy(s, 0, 1).wait_send()
                pl.semaphore_wait(slot_free.at[0], 1)

            out_s[k] = base().astype(BF16)

            @pl.when(place == 3)
            def _():
                part_copy(s, 0, 2).start()

            @pl.when(place == 0)
            def _():
                part_copy(s, 1, 1).start()

        @pl.when(place == 2)
        def _():
            @pl.when(s >= K)
            def _():
                part_copy(s, 0, 1).wait_send()
                pl.semaphore_wait(slot_free.at[0], 1)

            part_copy(s, 0, 1).wait_recv()
            out_s[k] = (base() + part_s[0, k].astype(F32)).astype(BF16)

            @pl.when(s < NS - K)
            def _():
                free_slot(0, 3)

            part_copy(s, 0, 1).start()

        @pl.when(place == 1)
        def _():
            @pl.when(s >= K)
            def _():
                for c in owner_sends(s)[:3]:
                    c.wait_send()
                fin_here(s).wait()

            part_copy(s, 0, 1).wait_recv()
            part_copy(s, 1, 1).wait_recv()
            out_s[k] = (base() + part_s[0, k].astype(F32) + part_s[1, k].astype(F32)).astype(BF16)

            @pl.when(s < NS - K)
            def _():
                free_slot(0, 2)
                free_slot(0, 0)

            for c in owner_sends(s):
                c.start()

        @pl.when((r == PER - 1) & (s < NS - 2 * PER))
        def _():
            pl.semaphore_signal(got_free, inc=1, device_id=to_mate, device_id_type=MESH)

    def forward(s):
        @pl.when(place != 1)
        def _():
            fin_copy(s, 0, 0).wait_recv()
            fwd_pair_copy(s).start()

            @pl.when(place == 2)
            def _():
                fwd_line_copy(s).start()

    def tick(n):
        @pl.when((n >= lead) & (n < NS + lead))
        def _():
            combine(n - lead)

        @pl.when((n >= late) & (n < NS + late))
        def _():
            forward(n - late)

    lane = lax.broadcasted_iota(jnp.int32, (CH, HEAD), 1)
    e = HEAD**-0.5 * LOG2E

    def turn(t, i):
        cs = cs_ref[pl.ds(pl.multiple_of(i * CH, CH), CH), :]
        swap = pltpu.roll(cs, HEAD // 2, 1)
        cos = jnp.where(lane < HEAD // 2, cs, swap)
        sin = jnp.where(lane < HEAD // 2, -swap, cs)
        t = t.astype(BF16).astype(F32)
        return (t * cos + pltpu.roll(t, HEAD // 2, 1) * sin).astype(BF16)

    def attend(i, g):
        top_s[...] = jnp.full(top_s.shape, NEG, F32)
        mix_s[...] = jnp.zeros(mix_s.shape, F32)

        def block(start, nk, masked):
            start = pl.multiple_of(start, CH)
            keys, values = k_s[pl.ds(start, nk), :], vt_s[:, pl.ds(start, nk)]
            scores = [_dot(keys, q_s[g * z.piece + h], 1, 1) for h in range(z.piece)]
            if masked:
                ok = lax.broadcasted_iota(jnp.int32, (nk, CH), 1) + (nk - CH) >= lax.broadcasted_iota(jnp.int32, (nk, CH), 0)
            weights, keeps = [], []
            for h, s in enumerate(scores):
                if masked:
                    s = jnp.where(ok, s, HIDDEN)
                old = top_s[h:h + 1, :]
                top = jnp.maximum(old, s.max(axis=0, keepdims=True))
                top_s[h:h + 1, :] = top
                weights.append(jnp.exp2((s - top) * e).astype(BF16))
                keeps.append(jnp.exp2((old - top) * e))
            for h, (p, keep) in enumerate(zip(weights, keeps)):
                mix_s[h] = mix_s[h] * keep + _dot(values, p, 1, 0)

        lax.fori_loop(0, lax.div(i, 2), lambda j, _: block(j * 2 * CH, 2 * CH, False), None)

        @pl.when(lax.rem(i, 2) == 1)
        def _():
            block((i - 1) * CH, 2 * CH, True)

        @pl.when(lax.rem(i, 2) == 0)
        def _():
            block(i * CH, CH, True)

        for h in range(z.piece):
            total = mix_s[h, HEAD:HEAD + 1, :]
            got = (mix_s[h, :HEAD, :] * (1 / total)).T.astype(BF16)
            seen_s[:, pl.ds(pl.multiple_of((g * z.piece + h) * HEAD, HEAD), HEAD)] = got

    def body(i, _):
        b = lax.rem(i, 2)
        n0 = (i - 1) * PER
        first = i == 0
        x_copy(i).wait()

        @pl.when(i + 1 < NCH)
        def _():
            x_copy(i + 1).start()

        NB = 16 if CH % 16 == 0 else 8

        def norm(r, _):
            rows = pl.ds(pl.multiple_of(r * NB, NB), NB)
            wide = x_s[b, rows, :].astype(F32)
            scale = lax.rsqrt(jnp.mean(wide * wide, -1, keepdims=True) + 1e-6)
            a_s[rows, :] = (wide * scale * gain_ref[...].astype(F32)).astype(BF16)

        lax.fori_loop(0, CH // NB, norm, None)

        @pl.when(first)
        def _():
            wk_copy.wait()
            wv_copy.wait()

        kv = _dot(a_s[...], wkv_s[...])
        here = pl.ds(pl.multiple_of(i * CH, CH), CH)
        k_s[here, :] = turn(kv[:, :HEAD], i)
        vt_s[:HEAD, here] = kv[:, HEAD:].T.astype(BF16)

        def project(j, _):
            @pl.when(first)
            def _():
                wq_copy(j).wait()

            t = _dot(a_s[...], wq_s[j])
            q_s[2 * j] = turn(t[:, :HEAD], i)
            q_s[2 * j + 1] = turn(t[:, HEAD:], i)

            @pl.when(lax.rem(j, 3) == 2)
            def _():
                tick(n0 + lax.div(j, 3))

        lax.fori_loop(0, pairs, project, None)

        @pl.when(first)
        def _():
            for j in range(8):
                wo_copy(j).start()

        def heads(g, _):
            attend(i, g)
            tick(n0 + 2 + g)

        lax.fori_loop(0, z.heads // z.piece, heads, None)

        @pl.when(i >= 2)
        def _():
            give_copy(i).wait_send()

        def out_mate(t, _):
            j = t + 4 * (1 - core)

            @pl.when(first)
            def _():
                wo_copy(j).wait()

            cols = pl.ds(pl.multiple_of(t * z.os, z.os), z.os)
            give_s[b, :, cols] = _dot(seen_s[...], wo_s[j]).astype(BF16)

        lax.fori_loop(0, 4, out_mate, None)

        @pl.when(i >= 2)
        def _():
            pl.semaphore_wait(got_free, 1)

        give_copy(i).start()
        tick(n0 + 6)

        def out_own(t, _):
            j = t + 4 * core

            @pl.when(first)
            def _():
                wo_copy(j).wait()

            cols = pl.ds(pl.multiple_of(t * z.os, z.os), z.os)
            x_cols = pl.ds(pl.multiple_of(j * z.os, z.os), z.os)
            got = _dot(seen_s[...], wo_s[j])

            @pl.when(place == 1)
            def _():
                own_s[b, :, cols] = got + x_s[b, :, x_cols].astype(F32)

            @pl.when(place != 1)
            def _():
                own_s[b, :, cols] = got

        lax.fori_loop(0, 4, out_own, None)
        tick(n0 + 7)

    lax.fori_loop(0, NCH, body, None)
    lax.fori_loop((NCH - 1) * PER, NS + 4 * D, lambda n, _: tick(n), None)

    for i in range(max(NCH - 2, 0), NCH):
        give_copy(i).wait_send()

    def drain(s, _):
        @pl.when(place != 1)
        def _():
            part_copy(s, 0, 1).wait_send()

        @pl.when(place == 1)
        def _():
            for c in owner_sends(s)[:3]:
                c.wait_send()
            fin_here(s).wait()

    lax.fori_loop(NS - K, NS, drain, None)

    def last(s, _):
        pltpu.make_async_remote_copy(piece_of_y(s, mate_cols), piece_of_y(s, mate_cols), fwd_sem.at[0, s], pair_sem.at[s],
                                     device_id=to_mate, device_id_type=MESH).wait_recv()

        @pl.when(place != 1)
        def _():
            fwd_pair_copy(s).wait_send()

        @pl.when(place == 2)
        def _():
            fwd_line_copy(s).wait_send()

    lax.fori_loop(0, NS, last, None)


def layer(z, x, gain, wq, wk, wv, wo):
    half = HEAD // 2
    angle = np.arange(z.rows)[:, None] * (float(THETA) ** (-np.arange(half) / half))[None]
    cs = jnp.asarray(np.concatenate([np.cos(angle), np.sin(angle)], 1), F32)
    any_, vmem = pl.BlockSpec(memory_space=pl.ANY), pl.BlockSpec(memory_space=pltpu.VMEM)
    dma = pltpu.SemaphoreType.DMA
    pairs = z.heads // 2
    flops = 2 * z.rows * z.d * (2 * z.heads + 2) * HEAD + 2 * z.rows * z.rows * z.heads * HEAD
    return pl.pallas_call(
        functools.partial(_kernel, z),
        out_shape=jax.ShapeDtypeStruct((z.rows, z.d), BF16),
        in_specs=[any_, vmem, vmem, any_, any_, any_, any_],
        out_specs=any_,
        scratch_shapes=[
            pltpu.VMEM((pairs, z.d, 2 * HEAD), BF16),
            pltpu.VMEM((z.d, 2 * HEAD), BF16),
            pltpu.VMEM((8, z.heads * HEAD, z.os), BF16),
            pltpu.VMEM((2, z.chunk, z.d), BF16),
            pltpu.VMEM((z.chunk, z.d), BF16),
            pltpu.VMEM((z.heads, z.chunk, HEAD), BF16),
            pltpu.VMEM((z.rows, HEAD), BF16),
            pltpu.VMEM((HEAD + 8, z.rows), BF16),
            pltpu.VMEM((z.chunk, z.heads * HEAD), BF16),
            pltpu.VMEM((8, z.chunk), F32),
            pltpu.VMEM((z.piece, HEAD + 8, z.chunk), F32),
            pltpu.VMEM((2, z.chunk, z.half), F32),
            pltpu.VMEM((2, z.chunk, z.half), BF16),
            pltpu.VMEM((2, z.chunk, z.half), BF16),
            pltpu.VMEM((2, z.slots, z.sub, z.half), BF16),
            pltpu.VMEM((z.slots, z.sub, z.half), BF16),
            dma((pairs + 10,)),
            dma((2,)),
            dma((2,)),
            dma((2,)),
            dma((2, z.slots)),
            dma((4, z.slots)),
            dma((z.ns,)),
            dma((2, z.ns)),
            dma((z.ns,)),
            pltpu.SemaphoreType.REGULAR((1,)),
            pltpu.SemaphoreType.REGULAR,
        ],
        compiler_params=pltpu.CompilerParams(collective_id=0, has_side_effects=True, vmem_limit_bytes=60 * 2**20),
        cost_estimate=pl.CostEstimate(flops=flops, bytes_accessed=2**26, transcendentals=z.rows * z.rows * z.heads // 2),
        name="layer",
    )(x, gain.reshape(1, -1), cs, wq, wk, wv, wo)


def solution(mesh):
    def step(x, gain, wq, wk, wv, wo):
        return layer(Sizes(x.shape[0], x.shape[1], wq.shape[1] // HEAD), x, gain, wq, wk, wv, wo)

    tokens, columns = P("dp", None), P(None, "tp")
    return jax.shard_map(
        step,
        mesh=mesh,
        in_specs=(tokens, P(None), columns, columns, columns, P("tp", None)),
        out_specs=tokens,
        check_vma=False,
    )
```

```python
import functools

import jax
import jax.numpy as jnp
import numpy as np
from jax import lax
from jax.experimental import pallas as pl
from jax.experimental.pallas import tpu as pltpu
from jax.sharding import PartitionSpec as P

HEAD = 128
THETA = 10000
NEG = -1e30
HIDDEN = 2 * NEG
LOG2E = 1.4426950408889634
MESH = pl.DeviceIdType.MESH
F32, BF16 = jnp.float32, jnp.bfloat16


def _dot(a, b, ca=1, cb=0):
    return lax.dot_general(a, b, (((ca,), (cb,)), ((), ())), preferred_element_type=F32)


class Sizes:
    def __init__(self, rows, d, heads, chunk=256, sub=32, slots=8, hop=2, piece=6, norm_unroll=16):
        self.rows, self.d, self.heads = rows, d, heads
        self.chunk, self.sub, self.slots, self.hop, self.piece = chunk, sub, slots, hop, piece
        self.norm_unroll = norm_unroll
        self.chunks = rows // chunk
        self.per = chunk // sub
        self.ns = rows // sub
        self.half = d // 2
        self.os = d // 8


def _kernel(z, x_hbm, gain_ref, cs_ref, wq_hbm, wk_hbm, wv_hbm, wo_hbm, y_hbm,
            wq_s, wkv_s, wo_s, x_s, xr_s, a_s, q_s, k_s, vt_s, seen_s, top_s, mix_s, gain_s,
            own_s, give_s, got_s, part_s, out_s,
            w_sem, x_sem, xr_sem, give_sem, got_sem, part_sem, out_sem, fin_sem, fwd_sem, pair_sem, slot_free, got_free):
    CH, SUB, K, D, PER, NS, NCH = z.chunk, z.sub, z.slots, z.hop, z.per, z.ns, z.chunks
    half = z.half
    me = lax.axis_index("tp")
    core, line = lax.rem(me, 2), lax.div(me, 2)
    mate = me + 1 - 2 * core
    place = jnp.where(core == 0, line, 3 - line)

    def at(q):
        return {"tp": jnp.where(core == 0, 2 * q, 7 - 2 * q)}

    to_mate = {"tp": mate}
    mine = pl.multiple_of(core * half, half)
    theirs = pl.multiple_of((1 - core) * half, half)
    own_cols, mate_cols = pl.ds(mine, half), pl.ds(theirs, half)
    pairs = z.heads // 2
    barrier = pltpu.get_barrier_semaphore()
    for other in range(1, 8):
        pl.semaphore_signal(barrier, inc=1, device_id={"tp": lax.rem(me + other, 8)}, device_id_type=MESH)

    def x_copy(i):
        return pltpu.make_async_copy(x_hbm.at[pl.ds(i * CH, CH), :], x_s.at[lax.rem(i, 2)], x_sem.at[lax.rem(i, 2)])

    def xr_copy(i):
        return pltpu.make_async_copy(x_hbm.at[pl.ds(i * CH, CH), own_cols], xr_s, xr_sem)

    def wq_copy(j):
        return pltpu.make_async_copy(wq_hbm.at[:, pl.ds(j * 2 * HEAD, 2 * HEAD)], wq_s.at[j], w_sem.at[j])

    wk_copy = pltpu.make_async_copy(wk_hbm, wkv_s.at[:, pl.ds(0, HEAD)], w_sem.at[pairs])
    wv_copy = pltpu.make_async_copy(wv_hbm, wkv_s.at[:, pl.ds(HEAD, HEAD)], w_sem.at[pairs + 1])

    def wo_copy(j):
        return pltpu.make_async_copy(wo_hbm.at[:, pl.ds(j * z.os, z.os)], wo_s.at[j], w_sem.at[pairs + 2 + j])

    x_copy(0).start()
    wk_copy.start()
    wv_copy.start()
    for j in range(pairs):
        wq_copy(j).start()
    gain_s[...] = gain_ref[...].astype(F32).reshape(1, z.d)
    vt_s[HEAD:, :] = jnp.ones((8, z.rows), BF16)
    pl.semaphore_wait(barrier, 7)

    def give_copy(i):
        b = lax.rem(i, 2)
        return pltpu.make_async_remote_copy(give_s.at[b], got_s.at[b], give_sem.at[b], got_sem.at[b], device_id=to_mate, device_id_type=MESH)

    def part_copy(s, lane, q):
        k = lax.rem(s, K)
        return pltpu.make_async_remote_copy(out_s.at[k], part_s.at[lane, k], out_sem.at[0, k], part_sem.at[lane, k], device_id=at(q), device_id_type=MESH)

    def piece_of_y(s, cols):
        return y_hbm.at[pl.ds(s * SUB, SUB), cols]

    def fin_copy(s, n, q):
        k = lax.rem(s, K)
        return pltpu.make_async_remote_copy(out_s.at[k], piece_of_y(s, own_cols), out_sem.at[n, k], fin_sem.at[s], device_id=at(q), device_id_type=MESH)

    def fin_pair_copy(s):
        k = lax.rem(s, K)
        return pltpu.make_async_remote_copy(out_s.at[k], piece_of_y(s, own_cols), out_sem.at[2, k], pair_sem.at[s], device_id=to_mate, device_id_type=MESH)

    def fin_here(s):
        k = lax.rem(s, K)
        return pltpu.make_async_copy(out_s.at[k], piece_of_y(s, own_cols), out_sem.at[3, k])

    def fwd_pair_copy(s):
        return pltpu.make_async_remote_copy(piece_of_y(s, own_cols), piece_of_y(s, own_cols), fwd_sem.at[0, s], pair_sem.at[s], device_id=to_mate, device_id_type=MESH)

    def fwd_line_copy(s):
        return pltpu.make_async_remote_copy(piece_of_y(s, own_cols), piece_of_y(s, own_cols), fwd_sem.at[1, s], fin_sem.at[s], device_id=at(3), device_id_type=MESH)

    def owner_sends(s):
        return fin_copy(s, 0, 0), fin_copy(s, 1, 2), fin_pair_copy(s), fin_here(s)

    def free_slot(lane, q):
        pl.semaphore_signal(slot_free.at[lane], inc=1, device_id=at(q), device_id_type=MESH)

    lead = jnp.where(place == 2, D, jnp.where(place == 1, 2 * D, 0))
    late = jnp.where(place == 3, 4 * D, 3 * D)

    def combine(s):
        b, r, k = lax.rem(lax.div(s, PER), 2), lax.rem(s, PER), lax.rem(s, K)
        rows = pl.ds(pl.multiple_of(r * SUB, SUB), SUB)

        @pl.when(r == 0)
        def _():
            give_copy(lax.div(s, PER)).wait_recv()

        def base():
            return own_s[b, rows, :] + got_s[b, rows, :].astype(F32)

        @pl.when((place == 3) | (place == 0))
        def _():
            @pl.when(s >= K)
            def _():
                part_copy(s, 0, 1).wait_send()
                pl.semaphore_wait(slot_free.at[0], 1)

            out_s[k] = base().astype(BF16)

            @pl.when(place == 3)
            def _():
                part_copy(s, 0, 2).start()

            @pl.when(place == 0)
            def _():
                part_copy(s, 1, 1).start()

        @pl.when(place == 2)
        def _():
            @pl.when(s >= K)
            def _():
                part_copy(s, 0, 1).wait_send()
                pl.semaphore_wait(slot_free.at[0], 1)

            part_copy(s, 0, 1).wait_recv()
            out_s[k] = (base() + part_s[0, k].astype(F32)).astype(BF16)

            @pl.when(s < NS - K)
            def _():
                free_slot(0, 3)

            part_copy(s, 0, 1).start()

        @pl.when(place == 1)
        def _():
            @pl.when(s >= K)
            def _():
                for c in owner_sends(s)[:3]:
                    c.wait_send()
                fin_here(s).wait()

            part_copy(s, 0, 1).wait_recv()
            part_copy(s, 1, 1).wait_recv()
            out_s[k] = (base() + part_s[0, k].astype(F32) + part_s[1, k].astype(F32)).astype(BF16)

            @pl.when(s < NS - K)
            def _():
                free_slot(0, 2)
                free_slot(0, 0)

            for c in owner_sends(s):
                c.start()

        @pl.when((r == PER - 1) & (s < NS - 2 * PER))
        def _():
            pl.semaphore_signal(got_free, inc=1, device_id=to_mate, device_id_type=MESH)

    def forward(s):
        @pl.when(place != 1)
        def _():
            fin_copy(s, 0, 0).wait_recv()
            fwd_pair_copy(s).start()

            @pl.when(place == 2)
            def _():
                fwd_line_copy(s).start()

    def tick(n):
        @pl.when((n >= lead) & (n < NS + lead))
        def _():
            combine(n - lead)

        @pl.when((n >= late) & (n < NS + late))
        def _():
            forward(n - late)

    lane = lax.broadcasted_iota(jnp.int32, (CH, HEAD), 1)
    e = HEAD**-0.5 * LOG2E
    c_block = 10 * z.piece // 3

    def turn(t, i):
        cs = cs_ref[pl.ds(pl.multiple_of(i * CH, CH), CH), :]
        swap = pltpu.roll(cs, HEAD // 2, 1)
        cos = jnp.where(lane < HEAD // 2, cs, swap)
        sin = jnp.where(lane < HEAD // 2, -swap, cs)
        t = t.astype(BF16).astype(F32)
        return (t * cos + pltpu.roll(t, HEAD // 2, 1) * sin).astype(BF16)

    def attend(i, g, ticks, at_piece):
        top_s[...] = jnp.full(top_s.shape, NEG, F32)
        mix_s[...] = jnp.zeros(mix_s.shape, F32)

        def block(start, nk, masked):
            start = pl.multiple_of(start, CH)
            keys, values = k_s[pl.ds(start, nk), :], vt_s[:, pl.ds(start, nk)]
            scores = [_dot(keys, q_s[i, g * z.piece + h], 1, 1) for h in range(z.piece)]
            if masked:
                ok = lax.broadcasted_iota(jnp.int32, (nk, CH), 1) + (nk - CH) >= lax.broadcasted_iota(jnp.int32, (nk, CH), 0)
            weights, keeps = [], []
            for h, s in enumerate(scores):
                if masked:
                    s = jnp.where(ok, s, HIDDEN)
                old = top_s[h:h + 1, :]
                top = jnp.maximum(old, s.max(axis=0, keepdims=True))
                top_s[h:h + 1, :] = top
                weights.append(jnp.exp2((s - top) * e).astype(BF16))
                keeps.append(jnp.exp2((old - top) * e))
            for h, (p, keep) in enumerate(zip(weights, keeps)):
                mix_s[h] = mix_s[h] * keep + _dot(values, p, 1, 0)

        def whole(j, _):
            block(j * 2 * CH, 2 * CH, False)
            ticks(at_piece + j * 2 * c_block, at_piece + (j + 1) * 2 * c_block)

        lax.fori_loop(0, lax.div(i, 2), whole, None)

        @pl.when(lax.rem(i, 2) == 1)
        def _():
            block((i - 1) * CH, 2 * CH, True)

        @pl.when(lax.rem(i, 2) == 0)
        def _():
            block(i * CH, CH, True)

        for h in range(z.piece):
            total = mix_s[h, HEAD:HEAD + 1, :]
            got = (mix_s[h, :HEAD, :] * (1 / total)).T.astype(BF16)
            seen_s[:, pl.ds(pl.multiple_of((g * z.piece + h) * HEAD, HEAD), HEAD)] = got

    def qkv_done(i):
        return jnp.minimum(jnp.minimum(2 * i + 1, i + 3), NCH)

    def body(i, _):
        b = lax.rem(i, 2)
        first = i == 0
        c_from, c_to = jnp.where(first, 0, qkv_done(i - 1)), qkv_done(i)
        c_norm, c_strip, c_heads, c_out = 32, 16, c_block * i + c_block // 2, 11
        c_qkv = c_norm + pairs * c_strip
        at_heads = (c_to - c_from) * c_qkv
        at_out = at_heads + z.heads // z.piece * c_heads
        whole = at_out + 8 * c_out

        def ticks(before, after):
            def due(point):
                return jnp.minimum(1 + lax.div(point * PER, whole), PER)

            lo = jnp.where(before < 0, 0, due(before))
            hi = jnp.where(first, lo, due(after))
            lax.fori_loop(lo, hi, lambda n, _: tick((i - 1) * PER + n), None)

        @pl.when(place == 1)
        def _():
            xr_copy(i).start()

        ticks(-1, 0)

        def qkv(c, _):
            x_copy(c).wait()

            @pl.when(c + 1 < NCH)
            def _():
                x_copy(c + 1).start()

            NB = 16

            def norm(r, _):
                rows = pl.ds(pl.multiple_of(r * NB, NB), NB)
                wide = x_s[lax.rem(c, 2), rows, :].astype(F32)
                scale = lax.rsqrt(jnp.mean(wide * wide, -1, keepdims=True) + 1e-6)
                a_s[rows, :] = (wide * scale * gain_s[...]).astype(BF16)

            lax.fori_loop(0, CH // NB, norm, None, unroll=z.norm_unroll)

            @pl.when(c == 0)
            def _():
                wk_copy.wait()
                wv_copy.wait()

            kv = _dot(a_s[...], wkv_s[...])
            here = pl.ds(pl.multiple_of(c * CH, CH), CH)
            k_s[here, :] = turn(kv[:, :HEAD], c)
            vt_s[:HEAD, here] = kv[:, HEAD:].T.astype(BF16)
            start = (c - c_from) * c_qkv
            ticks(start, start + c_norm)

            def project(j, _):
                @pl.when(c == 0)
                def _():
                    wq_copy(j).wait()

                    @pl.when(j >= 1)
                    def _():
                        wo_copy(lax.rem(j - 1 + 4 * (1 - core), 8)).start()

                t = _dot(a_s[...], wq_s[j])
                q_s[c, 2 * j] = turn(t[:, :HEAD], c)
                q_s[c, 2 * j + 1] = turn(t[:, HEAD:], c)
                ticks(start + c_norm + j * c_strip, start + c_norm + (j + 1) * c_strip)

            lax.fori_loop(0, pairs, project, None)

        lax.fori_loop(c_from, c_to, qkv, None)

        @pl.when(first)
        def _():
            for j in range(pairs - 1, 8):
                wo_copy(lax.rem(j + 4 * (1 - core), 8)).start()

        def heads(g, _):
            at_piece = at_heads + g * c_heads
            attend(i, g, ticks, at_piece)
            ticks(at_piece + lax.div(i, 2) * 2 * c_block, at_piece + c_heads)

        lax.fori_loop(0, z.heads // z.piece, heads, None)

        @pl.when(i >= 2)
        def _():
            give_copy(i).wait_send()

        def out_mate(t, _):
            j = t + 4 * (1 - core)

            @pl.when(first)
            def _():
                wo_copy(j).wait()

            cols = pl.ds(pl.multiple_of(t * z.os, z.os), z.os)
            give_s[b, :, cols] = _dot(seen_s[...], wo_s[j]).astype(BF16)
            ticks(at_out + t * c_out, at_out + (t + 1) * c_out)

        lax.fori_loop(0, 4, out_mate, None)

        @pl.when(i >= 2)
        def _():
            pl.semaphore_wait(got_free, 1)

        give_copy(i).start()

        @pl.when(place == 1)
        def _():
            xr_copy(i).wait()

        def out_own(t, _):
            j = t + 4 * core

            @pl.when(first)
            def _():
                wo_copy(j).wait()

            cols = pl.ds(pl.multiple_of(t * z.os, z.os), z.os)
            got = _dot(seen_s[...], wo_s[j])

            @pl.when(place == 1)
            def _():
                own_s[b, :, cols] = got + xr_s[:, cols].astype(F32)

            @pl.when(place != 1)
            def _():
                own_s[b, :, cols] = got

            ticks(at_out + (t + 4) * c_out, at_out + (t + 5) * c_out)

        lax.fori_loop(0, 4, out_own, None)

    lax.fori_loop(0, NCH, body, None)
    lax.fori_loop((NCH - 1) * PER, NS + 4 * D, lambda n, _: tick(n), None)

    for i in range(max(NCH - 2, 0), NCH):
        give_copy(i).wait_send()

    def drain(s, _):
        @pl.when(place != 1)
        def _():
            part_copy(s, 0, 1).wait_send()

        @pl.when(place == 1)
        def _():
            for c in owner_sends(s)[:3]:
                c.wait_send()
            fin_here(s).wait()

    lax.fori_loop(NS - K, NS, drain, None)

    def last(s, _):
        pltpu.make_async_remote_copy(piece_of_y(s, mate_cols), piece_of_y(s, mate_cols), fwd_sem.at[0, s], pair_sem.at[s],
                                     device_id=to_mate, device_id_type=MESH).wait_recv()

        @pl.when(place != 1)
        def _():
            fwd_pair_copy(s).wait_send()

        @pl.when(place == 2)
        def _():
            fwd_line_copy(s).wait_send()

    lax.fori_loop(0, NS, last, None)


def layer(z, x, gain, wq, wk, wv, wo):
    half = HEAD // 2
    angle = np.arange(z.rows)[:, None] * (float(THETA) ** (-np.arange(half) / half))[None]
    cs = jnp.asarray(np.concatenate([np.cos(angle), np.sin(angle)], 1), F32)
    any_, vmem = pl.BlockSpec(memory_space=pl.ANY), pl.BlockSpec(memory_space=pltpu.VMEM)
    dma = pltpu.SemaphoreType.DMA
    pairs = z.heads // 2
    flops = 2 * z.rows * z.d * (2 * z.heads + 2) * HEAD + 2 * z.rows * z.rows * z.heads * HEAD
    return pl.pallas_call(
        functools.partial(_kernel, z),
        out_shape=jax.ShapeDtypeStruct((z.rows, z.d), BF16),
        in_specs=[any_, vmem, vmem, any_, any_, any_, any_],
        out_specs=any_,
        scratch_shapes=[
            pltpu.VMEM((pairs, z.d, 2 * HEAD), BF16),
            pltpu.VMEM((z.d, 2 * HEAD), BF16),
            pltpu.VMEM((8, z.heads * HEAD, z.os), BF16),
            pltpu.VMEM((2, z.chunk, z.d), BF16),
            pltpu.VMEM((z.chunk, z.half), BF16),
            pltpu.VMEM((z.chunk, z.d), BF16),
            pltpu.VMEM((z.chunks, z.heads, z.chunk, HEAD), BF16),
            pltpu.VMEM((z.rows, HEAD), BF16),
            pltpu.VMEM((HEAD + 8, z.rows), BF16),
            pltpu.VMEM((z.chunk, z.heads * HEAD), BF16),
            pltpu.VMEM((8, z.chunk), F32),
            pltpu.VMEM((z.piece, HEAD + 8, z.chunk), F32),
            pltpu.VMEM((1, z.d), F32),
            pltpu.VMEM((2, z.chunk, z.half), F32),
            pltpu.VMEM((2, z.chunk, z.half), BF16),
            pltpu.VMEM((2, z.chunk, z.half), BF16),
            pltpu.VMEM((2, z.slots, z.sub, z.half), BF16),
            pltpu.VMEM((z.slots, z.sub, z.half), BF16),
            dma((pairs + 10,)),
            dma((2,)),
            dma(()),
            dma((2,)),
            dma((2,)),
            dma((2, z.slots)),
            dma((4, z.slots)),
            dma((z.ns,)),
            dma((2, z.ns)),
            dma((z.ns,)),
            pltpu.SemaphoreType.REGULAR((1,)),
            pltpu.SemaphoreType.REGULAR,
        ],
        compiler_params=pltpu.CompilerParams(collective_id=0, has_side_effects=True, vmem_limit_bytes=60 * 2**20),
        cost_estimate=pl.CostEstimate(flops=flops, bytes_accessed=2**26, transcendentals=z.rows * z.rows * z.heads // 2),
        name="layer",
    )(x, gain, cs, wq, wk, wv, wo)


def _move(n, a_hbm, b_hbm, buf, in_sem, out_sem):
    rows = a_hbm.shape[0] // n

    def part(ref, i):
        return ref.at[pl.ds(i * rows, rows), :]

    for i in range(n):
        pltpu.make_async_copy(part(a_hbm, i), buf.at[i], in_sem.at[i]).start()
    for i in range(n):
        pltpu.make_async_copy(part(a_hbm, i), buf.at[i], in_sem.at[i]).wait()
        pltpu.make_async_copy(buf.at[i], part(b_hbm, i), out_sem.at[i]).start()
    for i in range(n):
        pltpu.make_async_copy(buf.at[i], part(b_hbm, i), out_sem.at[i]).wait()


def move(a, n=16):
    any_ = pl.BlockSpec(memory_space=pl.ANY)
    return pl.pallas_call(
        functools.partial(_move, n),
        out_shape=jax.ShapeDtypeStruct(a.shape, a.dtype),
        in_specs=[any_],
        out_specs=any_,
        scratch_shapes=[
            pltpu.VMEM((n, a.shape[0] // n, a.shape[1]), a.dtype),
            pltpu.SemaphoreType.DMA((n,)),
            pltpu.SemaphoreType.DMA((n,)),
        ],
        compiler_params=pltpu.CompilerParams(vmem_limit_bytes=60 * 2**20),
        cost_estimate=pl.CostEstimate(flops=a.size, bytes_accessed=4 * a.size, transcendentals=0),
        name="move",
    )(a)


def solution(mesh):
    def step(x, gain, wq, wk, wv, wo):
        return move(layer(Sizes(x.shape[0], x.shape[1], wq.shape[1] // HEAD), x, gain, wq, wk, wv, wo))

    tokens, columns = P("dp", None), P(None, "tp")
    return jax.shard_map(
        step,
        mesh=mesh,
        in_specs=(tokens, P(None), columns, columns, columns, P("tp", None)),
        out_specs=tokens,
        check_vma=False,
    )
```

```python
import functools

import jax
import jax.numpy as jnp
import numpy as np
from jax import lax
from jax.experimental import pallas as pl
from jax.experimental.pallas import tpu as pltpu
from jax.sharding import PartitionSpec as P

HEAD = 128
THETA = 10000
NEG = -1e30
HIDDEN = 2 * NEG
LOG2E = 1.4426950408889634
MESH = pl.DeviceIdType.MESH
F32, BF16 = jnp.float32, jnp.bfloat16


def _dot(a, b, ca=1, cb=0):
    return lax.dot_general(a, b, (((ca,), (cb,)), ((), ())), preferred_element_type=F32)


class Sizes:
    def __init__(self, rows, d, heads, chunk=256, sub=32, slots=8, hop=2, piece=6, norm_unroll=16):
        self.rows, self.d, self.heads = rows, d, heads
        self.chunk, self.sub, self.slots, self.hop, self.piece = chunk, sub, slots, hop, piece
        self.norm_unroll = norm_unroll
        self.chunks = rows // chunk
        self.per = chunk // sub
        self.ns = rows // sub
        self.half = d // 2
        self.os = d // 8


def _kernel(z, x_hbm, gain_hbm, cs_hbm, wq_hbm, wk_hbm, wv_hbm, wo_hbm, y_hbm,
            wq_s, wkv_s, wo_s, x_s, xr_s, a_s, q_s, k_s, vt_s, seen_s, top_s, mix_s, gain_b, gain_s, cs_s,
            own_s, give_s, got_s, part_s, out_s,
            w_sem, x_sem, xr_sem, give_sem, got_sem, part_sem, out_sem, fin_sem, fwd_sem, pair_sem, slot_free, got_free):
    CH, SUB, K, D, PER, NS, NCH = z.chunk, z.sub, z.slots, z.hop, z.per, z.ns, z.chunks
    half = z.half
    me = lax.axis_index("tp")
    core, line = lax.rem(me, 2), lax.div(me, 2)
    mate = me + 1 - 2 * core
    place = jnp.where(core == 0, line, 3 - line)

    def at(q):
        return {"tp": jnp.where(core == 0, 2 * q, 7 - 2 * q)}

    to_mate = {"tp": mate}
    mine = pl.multiple_of(core * half, half)
    theirs = pl.multiple_of((1 - core) * half, half)
    own_cols, mate_cols = pl.ds(mine, half), pl.ds(theirs, half)
    pairs = z.heads // 2
    barrier = pltpu.get_barrier_semaphore()
    for other in range(1, 8):
        pl.semaphore_signal(barrier, inc=1, device_id={"tp": lax.rem(me + other, 8)}, device_id_type=MESH)

    def x_copy(i):
        return pltpu.make_async_copy(x_hbm.at[pl.ds(i * CH, CH), :], x_s.at[lax.rem(i, 2)], x_sem.at[lax.rem(i, 2)])

    def xr_copy(i):
        return pltpu.make_async_copy(x_hbm.at[pl.ds(i * CH, CH), own_cols], xr_s, xr_sem)

    def wq_copy(j):
        return pltpu.make_async_copy(wq_hbm.at[:, pl.ds(j * 2 * HEAD, 2 * HEAD)], wq_s.at[j], w_sem.at[j])

    wk_copy = pltpu.make_async_copy(wk_hbm, wkv_s.at[:, pl.ds(0, HEAD)], w_sem.at[pairs])
    wv_copy = pltpu.make_async_copy(wv_hbm, wkv_s.at[:, pl.ds(HEAD, HEAD)], w_sem.at[pairs + 1])

    def wo_copy(j):
        return pltpu.make_async_copy(wo_hbm.at[:, pl.ds(j * z.os, z.os)], wo_s.at[j], w_sem.at[pairs + 2 + j])

    gain_copy = pltpu.make_async_copy(gain_hbm, gain_b, w_sem.at[pairs + 10])
    cs_copy = pltpu.make_async_copy(cs_hbm, cs_s, w_sem.at[pairs + 11])
    early = 3
    x_copy(0).start()
    gain_copy.start()
    wk_copy.start()
    wv_copy.start()
    cs_copy.start()
    for j in range(early):
        wq_copy(j).start()
    gain_copy.wait()
    gain_s[...] = gain_b[...].astype(F32).reshape(1, z.d)
    vt_s[HEAD:, :] = jnp.ones((8, z.rows), BF16)
    pl.semaphore_wait(barrier, 7)

    def give_copy(i):
        b = lax.rem(i, 2)
        return pltpu.make_async_remote_copy(give_s.at[b], got_s.at[b], give_sem.at[b], got_sem.at[b], device_id=to_mate, device_id_type=MESH)

    def part_copy(s, lane, q):
        k = lax.rem(s, K)
        return pltpu.make_async_remote_copy(out_s.at[k], part_s.at[lane, k], out_sem.at[0, k], part_sem.at[lane, k], device_id=at(q), device_id_type=MESH)

    def piece_of_y(s, cols):
        return y_hbm.at[pl.ds(s * SUB, SUB), cols]

    def fin_copy(s, n, q):
        k = lax.rem(s, K)
        return pltpu.make_async_remote_copy(out_s.at[k], piece_of_y(s, own_cols), out_sem.at[n, k], fin_sem.at[s], device_id=at(q), device_id_type=MESH)

    def fin_pair_copy(s):
        k = lax.rem(s, K)
        return pltpu.make_async_remote_copy(out_s.at[k], piece_of_y(s, own_cols), out_sem.at[2, k], pair_sem.at[s], device_id=to_mate, device_id_type=MESH)

    def fin_here(s):
        k = lax.rem(s, K)
        return pltpu.make_async_copy(out_s.at[k], piece_of_y(s, own_cols), out_sem.at[3, k])

    def fwd_pair_copy(s):
        return pltpu.make_async_remote_copy(piece_of_y(s, own_cols), piece_of_y(s, own_cols), fwd_sem.at[0, s], pair_sem.at[s], device_id=to_mate, device_id_type=MESH)

    def fwd_line_copy(s):
        return pltpu.make_async_remote_copy(piece_of_y(s, own_cols), piece_of_y(s, own_cols), fwd_sem.at[1, s], fin_sem.at[s], device_id=at(3), device_id_type=MESH)

    def owner_sends(s):
        return fin_copy(s, 0, 0), fin_copy(s, 1, 2), fin_pair_copy(s), fin_here(s)

    def free_slot(lane, q):
        pl.semaphore_signal(slot_free.at[lane], inc=1, device_id=at(q), device_id_type=MESH)

    lead = jnp.where(place == 2, D, jnp.where(place == 1, 2 * D, 0))
    late = jnp.where(place == 3, 4 * D, 3 * D)

    def combine(s):
        b, r, k = lax.rem(lax.div(s, PER), 2), lax.rem(s, PER), lax.rem(s, K)
        rows = pl.ds(pl.multiple_of(r * SUB, SUB), SUB)

        @pl.when(r == 0)
        def _():
            give_copy(lax.div(s, PER)).wait_recv()

        def base():
            return own_s[b, rows, :] + got_s[b, rows, :].astype(F32)

        @pl.when((place == 3) | (place == 0))
        def _():
            @pl.when(s >= K)
            def _():
                part_copy(s, 0, 1).wait_send()
                pl.semaphore_wait(slot_free.at[0], 1)

            out_s[k] = base().astype(BF16)

            @pl.when(place == 3)
            def _():
                part_copy(s, 0, 2).start()

            @pl.when(place == 0)
            def _():
                part_copy(s, 1, 1).start()

        @pl.when(place == 2)
        def _():
            @pl.when(s >= K)
            def _():
                part_copy(s, 0, 1).wait_send()
                pl.semaphore_wait(slot_free.at[0], 1)

            part_copy(s, 0, 1).wait_recv()
            out_s[k] = (base() + part_s[0, k].astype(F32)).astype(BF16)

            @pl.when(s < NS - K)
            def _():
                free_slot(0, 3)

            part_copy(s, 0, 1).start()

        @pl.when(place == 1)
        def _():
            @pl.when(s >= K)
            def _():
                for c in owner_sends(s)[:3]:
                    c.wait_send()
                fin_here(s).wait()

            part_copy(s, 0, 1).wait_recv()
            part_copy(s, 1, 1).wait_recv()
            out_s[k] = (base() + part_s[0, k].astype(F32) + part_s[1, k].astype(F32)).astype(BF16)

            @pl.when(s < NS - K)
            def _():
                free_slot(0, 2)
                free_slot(0, 0)

            for c in owner_sends(s):
                c.start()

        @pl.when((r == PER - 1) & (s < NS - 2 * PER))
        def _():
            pl.semaphore_signal(got_free, inc=1, device_id=to_mate, device_id_type=MESH)

    def forward(s):
        @pl.when(place != 1)
        def _():
            fin_copy(s, 0, 0).wait_recv()
            fwd_pair_copy(s).start()

            @pl.when(place == 2)
            def _():
                fwd_line_copy(s).start()

    def tick(n):
        @pl.when((n >= lead) & (n < NS + lead))
        def _():
            combine(n - lead)

        @pl.when((n >= late) & (n < NS + late))
        def _():
            forward(n - late)

    lane = lax.broadcasted_iota(jnp.int32, (CH, HEAD), 1)
    e = HEAD**-0.5 * LOG2E
    c_block = 10 * z.piece // 3

    def turn(t, i):
        cs = cs_s[pl.ds(pl.multiple_of(i * CH, CH), CH), :]
        swap = pltpu.roll(cs, HEAD // 2, 1)
        cos = jnp.where(lane < HEAD // 2, cs, swap)
        sin = jnp.where(lane < HEAD // 2, -swap, cs)
        t = t.astype(BF16).astype(F32)
        return (t * cos + pltpu.roll(t, HEAD // 2, 1) * sin).astype(BF16)

    def attend(i, g, ticks, at_piece):
        top_s[...] = jnp.full(top_s.shape, NEG, F32)
        mix_s[...] = jnp.zeros(mix_s.shape, F32)

        def block(start, nk, masked):
            start = pl.multiple_of(start, CH)
            keys, values = k_s[pl.ds(start, nk), :], vt_s[:, pl.ds(start, nk)]
            scores = [_dot(keys, q_s[i, g * z.piece + h], 1, 1) for h in range(z.piece)]
            if masked:
                ok = lax.broadcasted_iota(jnp.int32, (nk, CH), 1) + (nk - CH) >= lax.broadcasted_iota(jnp.int32, (nk, CH), 0)
            weights, keeps = [], []
            for h, s in enumerate(scores):
                if masked:
                    s = jnp.where(ok, s, HIDDEN)
                old = top_s[h:h + 1, :]
                top = jnp.maximum(old, s.max(axis=0, keepdims=True))
                top_s[h:h + 1, :] = top
                weights.append(jnp.exp2((s - top) * e).astype(BF16))
                keeps.append(jnp.exp2((old - top) * e))
            for h, (p, keep) in enumerate(zip(weights, keeps)):
                mix_s[h] = mix_s[h] * keep + _dot(values, p, 1, 0)

        def whole(j, _):
            block(j * 2 * CH, 2 * CH, False)
            ticks(at_piece + j * 2 * c_block, at_piece + (j + 1) * 2 * c_block)

        lax.fori_loop(0, lax.div(i, 2), whole, None)

        @pl.when(lax.rem(i, 2) == 1)
        def _():
            block((i - 1) * CH, 2 * CH, True)

        @pl.when(lax.rem(i, 2) == 0)
        def _():
            block(i * CH, CH, True)

        for h in range(z.piece):
            total = mix_s[h, HEAD:HEAD + 1, :]
            got = (mix_s[h, :HEAD, :] * (1 / total)).T.astype(BF16)
            seen_s[:, pl.ds(pl.multiple_of((g * z.piece + h) * HEAD, HEAD), HEAD)] = got

    def qkv_done(i):
        return jnp.minimum(jnp.minimum(2 * i + 1, i + 3), NCH)

    def body(i, _):
        b = lax.rem(i, 2)
        first = i == 0
        c_from, c_to = jnp.where(first, 0, qkv_done(i - 1)), qkv_done(i)
        c_norm, c_strip, c_heads, c_out = 32, 16, c_block * i + c_block // 2, 11
        c_qkv = c_norm + pairs * c_strip
        at_heads = (c_to - c_from) * c_qkv
        at_out = at_heads + z.heads // z.piece * c_heads
        whole = at_out + 8 * c_out

        def ticks(before, after):
            def due(point):
                return jnp.minimum(1 + lax.div(point * PER, whole), PER)

            lo = jnp.where(before < 0, 0, due(before))
            hi = jnp.where(first, lo, due(after))
            lax.fori_loop(lo, hi, lambda n, _: tick((i - 1) * PER + n), None)

        ticks(-1, 0)

        def qkv(c, _):
            x_copy(c).wait()

            @pl.when((c + 1 < NCH) & (c > 0))
            def _():
                x_copy(c + 1).start()

            NB = 16

            def norm(r, _):
                rows = pl.ds(pl.multiple_of(r * NB, NB), NB)
                wide = x_s[lax.rem(c, 2), rows, :].astype(F32)
                scale = lax.rsqrt(jnp.mean(wide * wide, -1, keepdims=True) + 1e-6)
                a_s[rows, :] = (wide * scale * gain_s[...]).astype(BF16)

            lax.fori_loop(0, CH // NB, norm, None, unroll=z.norm_unroll)

            @pl.when(c == 0)
            def _():
                wk_copy.wait()
                wv_copy.wait()
                cs_copy.wait()

            kv = _dot(a_s[...], wkv_s[...])
            here = pl.ds(pl.multiple_of(c * CH, CH), CH)
            k_s[here, :] = turn(kv[:, :HEAD], c)
            vt_s[:HEAD, here] = kv[:, HEAD:].T.astype(BF16)
            start = (c - c_from) * c_qkv
            ticks(start, start + c_norm)

            def project(j, _):
                @pl.when(c == 0)
                def _():
                    wq_copy(j).wait()

                    @pl.when(j + early < pairs)
                    def _():
                        wq_copy(j + early).start()

                    @pl.when(j + early >= pairs)
                    def _():
                        wo_copy(lax.rem(j + early - pairs + 4 * (1 - core), 8)).start()

                t = _dot(a_s[...], wq_s[j])
                q_s[c, 2 * j] = turn(t[:, :HEAD], c)
                q_s[c, 2 * j + 1] = turn(t[:, HEAD:], c)
                ticks(start + c_norm + j * c_strip, start + c_norm + (j + 1) * c_strip)

            lax.fori_loop(0, pairs, project, None)

        lax.fori_loop(c_from, c_to, qkv, None)

        @pl.when(first)
        def _():
            for j in range(early, 6):
                wo_copy(lax.rem(j + 4 * (1 - core), 8)).start()

        def heads(g, _):
            at_piece = at_heads + g * c_heads
            attend(i, g, ticks, at_piece)
            ticks(at_piece + lax.div(i, 2) * 2 * c_block, at_piece + c_heads)

        lax.fori_loop(0, z.heads // z.piece, heads, None)

        @pl.when(place == 1)
        def _():
            xr_copy(i).start()

        @pl.when(i >= 2)
        def _():
            give_copy(i).wait_send()

        def out_mate(t, _):
            j = t + 4 * (1 - core)

            @pl.when(first)
            def _():
                wo_copy(j).wait()

                @pl.when(t < 2)
                def _():
                    wo_copy(lax.rem(t + 6 + 4 * (1 - core), 8)).start()

                @pl.when(t == 2)
                def _():
                    x_copy(1).start()

            cols = pl.ds(pl.multiple_of(t * z.os, z.os), z.os)
            give_s[b, :, cols] = _dot(seen_s[...], wo_s[j]).astype(BF16)
            ticks(at_out + t * c_out, at_out + (t + 1) * c_out)

        lax.fori_loop(0, 4, out_mate, None)

        @pl.when(i >= 2)
        def _():
            pl.semaphore_wait(got_free, 1)

        give_copy(i).start()

        @pl.when(place == 1)
        def _():
            xr_copy(i).wait()

        def out_own(t, _):
            j = t + 4 * core

            @pl.when(first)
            def _():
                wo_copy(j).wait()

            cols = pl.ds(pl.multiple_of(t * z.os, z.os), z.os)
            got = _dot(seen_s[...], wo_s[j])

            @pl.when(place == 1)
            def _():
                own_s[b, :, cols] = got + xr_s[:, cols].astype(F32)

            @pl.when(place != 1)
            def _():
                own_s[b, :, cols] = got

            ticks(at_out + (t + 4) * c_out, at_out + (t + 5) * c_out)

        lax.fori_loop(0, 4, out_own, None)

    lax.fori_loop(0, NCH, body, None)
    lax.fori_loop((NCH - 1) * PER, NS + 4 * D, lambda n, _: tick(n), None)

    for i in range(max(NCH - 2, 0), NCH):
        give_copy(i).wait_send()

    def drain(s, _):
        @pl.when(place != 1)
        def _():
            part_copy(s, 0, 1).wait_send()

        @pl.when(place == 1)
        def _():
            for c in owner_sends(s)[:3]:
                c.wait_send()
            fin_here(s).wait()

    lax.fori_loop(NS - K, NS, drain, None)

    def last(s, _):
        pltpu.make_async_remote_copy(piece_of_y(s, mate_cols), piece_of_y(s, mate_cols), fwd_sem.at[0, s], pair_sem.at[s],
                                     device_id=to_mate, device_id_type=MESH).wait_recv()

        @pl.when(place != 1)
        def _():
            fwd_pair_copy(s).wait_send()

        @pl.when(place == 2)
        def _():
            fwd_line_copy(s).wait_send()

    lax.fori_loop(0, NS, last, None)


def layer(z, x, gain, wq, wk, wv, wo):
    half = HEAD // 2
    angle = np.arange(z.rows)[:, None] * (float(THETA) ** (-np.arange(half) / half))[None]
    cs = jnp.asarray(np.concatenate([np.cos(angle), np.sin(angle)], 1), F32)
    any_ = pl.BlockSpec(memory_space=pl.ANY)
    dma = pltpu.SemaphoreType.DMA
    pairs = z.heads // 2
    flops = 2 * z.rows * z.d * (2 * z.heads + 2) * HEAD + 2 * z.rows * z.rows * z.heads * HEAD
    return pl.pallas_call(
        functools.partial(_kernel, z),
        out_shape=jax.ShapeDtypeStruct((z.rows, z.d), BF16),
        in_specs=[any_] * 7,
        out_specs=any_,
        scratch_shapes=[
            pltpu.VMEM((pairs, z.d, 2 * HEAD), BF16),
            pltpu.VMEM((z.d, 2 * HEAD), BF16),
            pltpu.VMEM((8, z.heads * HEAD, z.os), BF16),
            pltpu.VMEM((2, z.chunk, z.d), BF16),
            pltpu.VMEM((z.chunk, z.half), BF16),
            pltpu.VMEM((z.chunk, z.d), BF16),
            pltpu.VMEM((z.chunks, z.heads, z.chunk, HEAD), BF16),
            pltpu.VMEM((z.rows, HEAD), BF16),
            pltpu.VMEM((HEAD + 8, z.rows), BF16),
            pltpu.VMEM((z.chunk, z.heads * HEAD), BF16),
            pltpu.VMEM((8, z.chunk), F32),
            pltpu.VMEM((z.piece, HEAD + 8, z.chunk), F32),
            pltpu.VMEM((z.d,), BF16),
            pltpu.VMEM((1, z.d), F32),
            pltpu.VMEM((z.rows, HEAD), F32),
            pltpu.VMEM((2, z.chunk, z.half), F32),
            pltpu.VMEM((2, z.chunk, z.half), BF16),
            pltpu.VMEM((2, z.chunk, z.half), BF16),
            pltpu.VMEM((2, z.slots, z.sub, z.half), BF16),
            pltpu.VMEM((z.slots, z.sub, z.half), BF16),
            dma((pairs + 12,)),
            dma((2,)),
            dma(()),
            dma((2,)),
            dma((2,)),
            dma((2, z.slots)),
            dma((4, z.slots)),
            dma((z.ns,)),
            dma((2, z.ns)),
            dma((z.ns,)),
            pltpu.SemaphoreType.REGULAR((1,)),
            pltpu.SemaphoreType.REGULAR,
        ],
        compiler_params=pltpu.CompilerParams(collective_id=0, has_side_effects=True, vmem_limit_bytes=60 * 2**20),
        cost_estimate=pl.CostEstimate(flops=flops, bytes_accessed=2**26, transcendentals=z.rows * z.rows * z.heads // 2),
        name="layer",
    )(x, gain, cs, wq, wk, wv, wo)


def _move(n, a_hbm, b_hbm, buf, in_sem, out_sem):
    rows = a_hbm.shape[0] // n

    def part(ref, i):
        return ref.at[pl.ds(i * rows, rows), :]

    for i in range(n):
        pltpu.make_async_copy(part(a_hbm, i), buf.at[i], in_sem.at[i]).start()
    for i in range(n):
        pltpu.make_async_copy(part(a_hbm, i), buf.at[i], in_sem.at[i]).wait()
        pltpu.make_async_copy(buf.at[i], part(b_hbm, i), out_sem.at[i]).start()
    for i in range(n):
        pltpu.make_async_copy(buf.at[i], part(b_hbm, i), out_sem.at[i]).wait()


def move(a, n=16):
    any_ = pl.BlockSpec(memory_space=pl.ANY)
    return pl.pallas_call(
        functools.partial(_move, n),
        out_shape=jax.ShapeDtypeStruct(a.shape, a.dtype),
        in_specs=[any_],
        out_specs=any_,
        scratch_shapes=[
            pltpu.VMEM((n, a.shape[0] // n, a.shape[1]), a.dtype),
            pltpu.SemaphoreType.DMA((n,)),
            pltpu.SemaphoreType.DMA((n,)),
        ],
        compiler_params=pltpu.CompilerParams(vmem_limit_bytes=60 * 2**20),
        cost_estimate=pl.CostEstimate(flops=a.size, bytes_accessed=4 * a.size, transcendentals=0),
        name="move",
    )(a)


def solution(mesh):
    def step(x, gain, wq, wk, wv, wo):
        return move(layer(Sizes(x.shape[0], x.shape[1], wq.shape[1] // HEAD), x, gain, wq, wk, wv, wo))

    tokens, columns = P("dp", None), P(None, "tp")
    return jax.shard_map(
        step,
        mesh=mesh,
        in_specs=(tokens, P(None), columns, columns, columns, P("tp", None)),
        out_specs=tokens,
        check_vma=False,
    )
```

```python
import functools

import jax
import jax.numpy as jnp
import numpy as np
from jax import lax
from jax.experimental import pallas as pl
from jax.experimental.pallas import tpu as pltpu
from jax.sharding import PartitionSpec as P

HEAD = 128
THETA = 10000
NEG = -1e30
HIDDEN = 2 * NEG
LOG2E = 1.4426950408889634
MESH = pl.DeviceIdType.MESH
F32, BF16 = jnp.float32, jnp.bfloat16


def _dot(a, b, ca=1, cb=0):
    return lax.dot_general(a, b, (((ca,), (cb,)), ((), ())), preferred_element_type=F32)


class Sizes:
    def __init__(self, rows, d, heads, chunk=256, sub=32, slots=8, hop=2, piece=6, norm_unroll=16):
        self.rows, self.d, self.heads = rows, d, heads
        self.chunk, self.sub, self.slots, self.hop, self.piece = chunk, sub, slots, hop, piece
        self.norm_unroll = norm_unroll
        self.chunks = rows // chunk
        self.per = chunk // sub
        self.ns = rows // sub
        self.half = d // 2
        self.os = d // 8


def _kernel(z, x_hbm, gain_hbm, cs_hbm, wq_hbm, wk_hbm, wv_hbm, wo_hbm, y_hbm,
            wq_s, wkv_s, wo_s, x_s, xr_s, a_s, q_s, k_s, vt_s, seen_s, top_s, mix_s, gain_b, gain_s, cs_s,
            own_s, give_s, got_s, part_s, out_s,
            w_sem, x_sem, xr_sem, give_sem, got_sem, part_sem, out_sem, fin_sem, fwd_sem, pair_sem, slot_free, got_free):
    CH, SUB, K, D, PER, NS, NCH = z.chunk, z.sub, z.slots, z.hop, z.per, z.ns, z.chunks
    half = z.half
    me = lax.axis_index("tp")
    core, line = lax.rem(me, 2), lax.div(me, 2)
    mate = me + 1 - 2 * core
    place = jnp.where(core == 0, line, 3 - line)

    def at(q):
        return {"tp": jnp.where(core == 0, 2 * q, 7 - 2 * q)}

    to_mate = {"tp": mate}
    mine = pl.multiple_of(core * half, half)
    theirs = pl.multiple_of((1 - core) * half, half)
    own_cols, mate_cols = pl.ds(mine, half), pl.ds(theirs, half)
    pairs = z.heads // 2
    barrier = pltpu.get_barrier_semaphore()
    for other in range(1, 8):
        pl.semaphore_signal(barrier, inc=1, device_id={"tp": lax.rem(me + other, 8)}, device_id_type=MESH)

    def x_copy(i):
        return pltpu.make_async_copy(x_hbm.at[pl.ds(i * CH, CH), :], x_s.at[lax.rem(i, 2)], x_sem.at[lax.rem(i, 2)])

    def xr_copy(i):
        return pltpu.make_async_copy(x_hbm.at[pl.ds(i * CH, CH), own_cols], xr_s, xr_sem)

    def wq_copy(j):
        return pltpu.make_async_copy(wq_hbm.at[:, pl.ds(j * 2 * HEAD, 2 * HEAD)], wq_s.at[j], w_sem.at[j])

    wk_copy = pltpu.make_async_copy(wk_hbm, wkv_s.at[:, pl.ds(0, HEAD)], w_sem.at[pairs])
    wv_copy = pltpu.make_async_copy(wv_hbm, wkv_s.at[:, pl.ds(HEAD, HEAD)], w_sem.at[pairs + 1])

    def wo_copy(j):
        return pltpu.make_async_copy(wo_hbm.at[:, pl.ds(j * z.os, z.os)], wo_s.at[j], w_sem.at[pairs + 2 + j])

    gain_copy = pltpu.make_async_copy(gain_hbm, gain_b, w_sem.at[pairs + 10])
    cs_copy = pltpu.make_async_copy(cs_hbm, cs_s, w_sem.at[pairs + 11])
    early = 3
    x_copy(0).start()
    gain_copy.start()
    wk_copy.start()
    wv_copy.start()
    cs_copy.start()
    for j in range(early):
        wq_copy(j).start()
    gain_copy.wait()
    gain_s[...] = gain_b[...].astype(F32).reshape(1, z.d)
    vt_s[HEAD:, :] = jnp.ones((8, z.rows), BF16)
    pl.semaphore_wait(barrier, 7)

    def give_copy(i):
        b = lax.rem(i, 2)
        return pltpu.make_async_remote_copy(give_s.at[b], got_s.at[b], give_sem.at[b], got_sem.at[b], device_id=to_mate, device_id_type=MESH)

    def part_copy(s, lane, q):
        k = lax.rem(s, K)
        return pltpu.make_async_remote_copy(out_s.at[k], part_s.at[lane, k], out_sem.at[0, k], part_sem.at[lane, k], device_id=at(q), device_id_type=MESH)

    def piece_of_y(s, cols):
        return y_hbm.at[pl.ds(s * SUB, SUB), cols]

    def fin_copy(s, n, q):
        k = lax.rem(s, K)
        return pltpu.make_async_remote_copy(out_s.at[k], piece_of_y(s, own_cols), out_sem.at[n, k], fin_sem.at[s], device_id=at(q), device_id_type=MESH)

    def fin_pair_copy(s):
        k = lax.rem(s, K)
        return pltpu.make_async_remote_copy(out_s.at[k], piece_of_y(s, own_cols), out_sem.at[2, k], pair_sem.at[s], device_id=to_mate, device_id_type=MESH)

    def fin_here(s):
        k = lax.rem(s, K)
        return pltpu.make_async_copy(out_s.at[k], piece_of_y(s, own_cols), out_sem.at[3, k])

    def fwd_pair_copy(s):
        return pltpu.make_async_remote_copy(piece_of_y(s, own_cols), piece_of_y(s, own_cols), fwd_sem.at[0, s], pair_sem.at[s], device_id=to_mate, device_id_type=MESH)

    def fwd_line_copy(s):
        return pltpu.make_async_remote_copy(piece_of_y(s, own_cols), piece_of_y(s, own_cols), fwd_sem.at[1, s], fin_sem.at[s], device_id=at(3), device_id_type=MESH)

    def owner_sends(s):
        return fin_copy(s, 1, 2), fin_copy(s, 0, 0), fin_pair_copy(s), fin_here(s)

    def free_slot(lane, q):
        pl.semaphore_signal(slot_free.at[lane], inc=1, device_id=at(q), device_id_type=MESH)

    lead = jnp.where(place == 2, D, jnp.where(place == 1, 2 * D, 0))
    late = jnp.where(place == 3, 4 * D, 3 * D)

    def combine(s):
        b, r, k = lax.rem(lax.div(s, PER), 2), lax.rem(s, PER), lax.rem(s, K)
        rows = pl.ds(pl.multiple_of(r * SUB, SUB), SUB)

        @pl.when(r == 0)
        def _():
            give_copy(lax.div(s, PER)).wait_recv()

        def base():
            return own_s[b, rows, :] + got_s[b, rows, :].astype(F32)

        @pl.when((place == 3) | (place == 0))
        def _():
            @pl.when(s >= K)
            def _():
                part_copy(s, 0, 1).wait_send()
                pl.semaphore_wait(slot_free.at[0], 1)

            out_s[k] = base().astype(BF16)

            @pl.when(place == 3)
            def _():
                part_copy(s, 0, 2).start()

            @pl.when(place == 0)
            def _():
                part_copy(s, 1, 1).start()

        @pl.when(place == 2)
        def _():
            @pl.when(s >= K)
            def _():
                part_copy(s, 0, 1).wait_send()
                pl.semaphore_wait(slot_free.at[0], 1)

            part_copy(s, 0, 1).wait_recv()
            out_s[k] = (base() + part_s[0, k].astype(F32)).astype(BF16)

            @pl.when(s < NS - K)
            def _():
                free_slot(0, 3)

            part_copy(s, 0, 1).start()

        @pl.when(place == 1)
        def _():
            @pl.when(s >= K)
            def _():
                for c in owner_sends(s)[:3]:
                    c.wait_send()
                fin_here(s).wait()

            part_copy(s, 0, 1).wait_recv()
            part_copy(s, 1, 1).wait_recv()
            out_s[k] = (base() + part_s[0, k].astype(F32) + part_s[1, k].astype(F32)).astype(BF16)

            @pl.when(s < NS - K)
            def _():
                free_slot(0, 2)
                free_slot(0, 0)

            for c in owner_sends(s):
                c.start()

        @pl.when((r == PER - 1) & (s < NS - 2 * PER))
        def _():
            pl.semaphore_signal(got_free, inc=1, device_id=to_mate, device_id_type=MESH)

    def forward(s):
        @pl.when(place != 1)
        def _():
            fin_copy(s, 0, 0).wait_recv()

            @pl.when(place == 2)
            def _():
                fwd_line_copy(s).start()

            fwd_pair_copy(s).start()

    def tick(n):
        @pl.when((n >= late) & (n < NS + late))
        def _():
            forward(n - late)

        @pl.when((n >= lead) & (n < NS + lead))
        def _():
            combine(n - lead)

    lane = lax.broadcasted_iota(jnp.int32, (CH, HEAD), 1)
    e = HEAD**-0.5 * LOG2E
    c_block = 10 * z.piece // 3

    def turn(t, i):
        cs = cs_s[pl.ds(pl.multiple_of(i * CH, CH), CH), :]
        swap = pltpu.roll(cs, HEAD // 2, 1)
        cos = jnp.where(lane < HEAD // 2, cs, swap)
        sin = jnp.where(lane < HEAD // 2, -swap, cs)
        t = t.astype(BF16).astype(F32)
        return (t * cos + pltpu.roll(t, HEAD // 2, 1) * sin).astype(BF16)

    def attend(i, g, ticks, at_piece):
        top_s[...] = jnp.full(top_s.shape, NEG, F32)
        mix_s[...] = jnp.zeros(mix_s.shape, F32)

        def block(start, nk, masked):
            start = pl.multiple_of(start, CH)
            keys, values = k_s[pl.ds(start, nk), :], vt_s[:, pl.ds(start, nk)]
            scores = [_dot(keys, q_s[i, g * z.piece + h], 1, 1) for h in range(z.piece)]
            if masked:
                ok = lax.broadcasted_iota(jnp.int32, (nk, CH), 1) + (nk - CH) >= lax.broadcasted_iota(jnp.int32, (nk, CH), 0)
            weights, keeps = [], []
            for h, s in enumerate(scores):
                if masked:
                    s = jnp.where(ok, s, HIDDEN)
                old = top_s[h:h + 1, :]
                top = jnp.maximum(old, s.max(axis=0, keepdims=True))
                top_s[h:h + 1, :] = top
                weights.append(jnp.exp2((s - top) * e).astype(BF16))
                keeps.append(jnp.exp2((old - top) * e))
            for h, (p, keep) in enumerate(zip(weights, keeps)):
                mix_s[h] = mix_s[h] * keep + _dot(values, p, 1, 0)

        def whole(j, _):
            block(j * 2 * CH, 2 * CH, False)
            ticks(at_piece + j * 2 * c_block, at_piece + (j + 1) * 2 * c_block)

        lax.fori_loop(0, lax.div(i, 2), whole, None)

        @pl.when(lax.rem(i, 2) == 1)
        def _():
            block((i - 1) * CH, 2 * CH, True)

        @pl.when(lax.rem(i, 2) == 0)
        def _():
            block(i * CH, CH, True)

        for h in range(z.piece):
            total = mix_s[h, HEAD:HEAD + 1, :]
            got = (mix_s[h, :HEAD, :] * (1 / total)).T.astype(BF16)
            seen_s[:, pl.ds(pl.multiple_of((g * z.piece + h) * HEAD, HEAD), HEAD)] = got

    def qkv_done(i):
        return jnp.minimum(jnp.minimum(2 * i + 1, i + 3), NCH)

    def body(i, _):
        b = lax.rem(i, 2)
        first = i == 0
        c_from, c_to = jnp.where(first, 0, qkv_done(i - 1)), qkv_done(i)
        c_norm, c_strip, c_heads, c_out = 32, 16, c_block * i + c_block // 2, 11
        c_qkv = c_norm + pairs * c_strip
        at_heads = (c_to - c_from) * c_qkv
        at_out = at_heads + z.heads // z.piece * c_heads
        whole = at_out + 8 * c_out

        def ticks(before, after):
            def due(point):
                return jnp.minimum(1 + lax.div(point * PER, whole), PER)

            lo = jnp.where(before < 0, 0, due(before))
            hi = jnp.where(first, lo, due(after))
            lax.fori_loop(lo, hi, lambda n, _: tick((i - 1) * PER + n), None)

        ticks(-1, 0)

        def qkv(c, _):
            x_copy(c).wait()

            @pl.when((c + 1 < NCH) & (c > 0))
            def _():
                x_copy(c + 1).start()

            NB = 16

            def norm(r, _):
                rows = pl.ds(pl.multiple_of(r * NB, NB), NB)
                wide = x_s[lax.rem(c, 2), rows, :].astype(F32)
                scale = lax.rsqrt(jnp.mean(wide * wide, -1, keepdims=True) + 1e-6)
                a_s[rows, :] = (wide * scale * gain_s[...]).astype(BF16)

            lax.fori_loop(0, CH // NB, norm, None, unroll=z.norm_unroll)

            @pl.when(c == 0)
            def _():
                wk_copy.wait()
                wv_copy.wait()
                cs_copy.wait()

            kv = _dot(a_s[...], wkv_s[...])
            here = pl.ds(pl.multiple_of(c * CH, CH), CH)
            k_s[here, :] = turn(kv[:, :HEAD], c)
            vt_s[:HEAD, here] = kv[:, HEAD:].T.astype(BF16)
            start = (c - c_from) * c_qkv
            ticks(start, start + c_norm)

            def project(j, _):
                @pl.when(c == 0)
                def _():
                    wq_copy(j).wait()

                    @pl.when(j + early < pairs)
                    def _():
                        wq_copy(j + early).start()

                    @pl.when(j + early >= pairs)
                    def _():
                        wo_copy(lax.rem(j + early - pairs + 4 * (1 - core), 8)).start()

                t = _dot(a_s[...], wq_s[j])
                q_s[c, 2 * j] = turn(t[:, :HEAD], c)
                q_s[c, 2 * j + 1] = turn(t[:, HEAD:], c)
                ticks(start + c_norm + j * c_strip, start + c_norm + (j + 1) * c_strip)

            lax.fori_loop(0, pairs, project, None)

        lax.fori_loop(c_from, c_to, qkv, None)

        @pl.when(first)
        def _():
            for j in range(early, 6):
                wo_copy(lax.rem(j + 4 * (1 - core), 8)).start()

        def heads(g, _):
            at_piece = at_heads + g * c_heads
            attend(i, g, ticks, at_piece)
            ticks(at_piece + lax.div(i, 2) * 2 * c_block, at_piece + c_heads)

        lax.fori_loop(0, z.heads // z.piece, heads, None)

        @pl.when(place == 1)
        def _():
            xr_copy(i).start()

        @pl.when(i >= 2)
        def _():
            give_copy(i).wait_send()

        def out_mate(t, _):
            j = t + 4 * (1 - core)

            @pl.when(first)
            def _():
                wo_copy(j).wait()

                @pl.when(t < 2)
                def _():
                    wo_copy(lax.rem(t + 6 + 4 * (1 - core), 8)).start()

                @pl.when(t == 2)
                def _():
                    x_copy(1).start()

            cols = pl.ds(pl.multiple_of(t * z.os, z.os), z.os)
            give_s[b, :, cols] = _dot(seen_s[...], wo_s[j]).astype(BF16)
            ticks(at_out + t * c_out, at_out + (t + 1) * c_out)

        lax.fori_loop(0, 4, out_mate, None)

        @pl.when(i >= 2)
        def _():
            pl.semaphore_wait(got_free, 1)

        give_copy(i).start()

        @pl.when(place == 1)
        def _():
            xr_copy(i).wait()

        def out_own(t, _):
            j = t + 4 * core

            @pl.when(first)
            def _():
                wo_copy(j).wait()

            cols = pl.ds(pl.multiple_of(t * z.os, z.os), z.os)
            got = _dot(seen_s[...], wo_s[j])

            @pl.when(place == 1)
            def _():
                own_s[b, :, cols] = got + xr_s[:, cols].astype(F32)

            @pl.when(place != 1)
            def _():
                own_s[b, :, cols] = got

            ticks(at_out + (t + 4) * c_out, at_out + (t + 5) * c_out)

        lax.fori_loop(0, 4, out_own, None)

    lax.fori_loop(0, NCH, body, None)
    lax.fori_loop((NCH - 1) * PER, NS + 4 * D, lambda n, _: tick(n), None)

    for i in range(max(NCH - 2, 0), NCH):
        give_copy(i).wait_send()

    def drain(s, _):
        @pl.when(place != 1)
        def _():
            part_copy(s, 0, 1).wait_send()

        @pl.when(place == 1)
        def _():
            for c in owner_sends(s)[:3]:
                c.wait_send()
            fin_here(s).wait()

    lax.fori_loop(NS - K, NS, drain, None)

    def last(s, _):
        pltpu.make_async_remote_copy(piece_of_y(s, mate_cols), piece_of_y(s, mate_cols), fwd_sem.at[0, s], pair_sem.at[s],
                                     device_id=to_mate, device_id_type=MESH).wait_recv()

        @pl.when(place != 1)
        def _():
            fwd_pair_copy(s).wait_send()

        @pl.when(place == 2)
        def _():
            fwd_line_copy(s).wait_send()

    lax.fori_loop(0, NS, last, None)


def layer(z, x, gain, wq, wk, wv, wo):
    half = HEAD // 2
    angle = np.arange(z.rows)[:, None] * (float(THETA) ** (-np.arange(half) / half))[None]
    cs = jnp.asarray(np.concatenate([np.cos(angle), np.sin(angle)], 1), F32)
    any_ = pl.BlockSpec(memory_space=pl.ANY)
    dma = pltpu.SemaphoreType.DMA
    pairs = z.heads // 2
    flops = 2 * z.rows * z.d * (2 * z.heads + 2) * HEAD + 2 * z.rows * z.rows * z.heads * HEAD
    return pl.pallas_call(
        functools.partial(_kernel, z),
        out_shape=jax.ShapeDtypeStruct((z.rows, z.d), BF16),
        in_specs=[any_] * 7,
        out_specs=any_,
        scratch_shapes=[
            pltpu.VMEM((pairs, z.d, 2 * HEAD), BF16),
            pltpu.VMEM((z.d, 2 * HEAD), BF16),
            pltpu.VMEM((8, z.heads * HEAD, z.os), BF16),
            pltpu.VMEM((2, z.chunk, z.d), BF16),
            pltpu.VMEM((z.chunk, z.half), BF16),
            pltpu.VMEM((z.chunk, z.d), BF16),
            pltpu.VMEM((z.chunks, z.heads, z.chunk, HEAD), BF16),
            pltpu.VMEM((z.rows, HEAD), BF16),
            pltpu.VMEM((HEAD + 8, z.rows), BF16),
            pltpu.VMEM((z.chunk, z.heads * HEAD), BF16),
            pltpu.VMEM((8, z.chunk), F32),
            pltpu.VMEM((z.piece, HEAD + 8, z.chunk), F32),
            pltpu.VMEM((z.d,), BF16),
            pltpu.VMEM((1, z.d), F32),
            pltpu.VMEM((z.rows, HEAD), F32),
            pltpu.VMEM((2, z.chunk, z.half), F32),
            pltpu.VMEM((2, z.chunk, z.half), BF16),
            pltpu.VMEM((2, z.chunk, z.half), BF16),
            pltpu.VMEM((2, z.slots, z.sub, z.half), BF16),
            pltpu.VMEM((z.slots, z.sub, z.half), BF16),
            dma((pairs + 12,)),
            dma((2,)),
            dma(()),
            dma((2,)),
            dma((2,)),
            dma((2, z.slots)),
            dma((4, z.slots)),
            dma((z.ns,)),
            dma((2, z.ns)),
            dma((z.ns,)),
            pltpu.SemaphoreType.REGULAR((1,)),
            pltpu.SemaphoreType.REGULAR,
        ],
        compiler_params=pltpu.CompilerParams(collective_id=0, has_side_effects=True, vmem_limit_bytes=60 * 2**20),
        cost_estimate=pl.CostEstimate(flops=flops, bytes_accessed=2**26, transcendentals=z.rows * z.rows * z.heads // 2),
        name="layer",
    )(x, gain, cs, wq, wk, wv, wo)


def _move(n, a_hbm, b_hbm, buf, in_sem, out_sem):
    rows = a_hbm.shape[0] // n

    def part(ref, i):
        return ref.at[pl.ds(i * rows, rows), :]

    for i in range(n):
        pltpu.make_async_copy(part(a_hbm, i), buf.at[i], in_sem.at[i]).start()
    for i in range(n):
        pltpu.make_async_copy(part(a_hbm, i), buf.at[i], in_sem.at[i]).wait()
        pltpu.make_async_copy(buf.at[i], part(b_hbm, i), out_sem.at[i]).start()
    for i in range(n):
        pltpu.make_async_copy(buf.at[i], part(b_hbm, i), out_sem.at[i]).wait()


def move(a, n=8):
    any_ = pl.BlockSpec(memory_space=pl.ANY)
    return pl.pallas_call(
        functools.partial(_move, n),
        out_shape=jax.ShapeDtypeStruct(a.shape, a.dtype),
        in_specs=[any_],
        out_specs=any_,
        scratch_shapes=[
            pltpu.VMEM((n, a.shape[0] // n, a.shape[1]), a.dtype),
            pltpu.SemaphoreType.DMA((n,)),
            pltpu.SemaphoreType.DMA((n,)),
        ],
        compiler_params=pltpu.CompilerParams(vmem_limit_bytes=60 * 2**20),
        cost_estimate=pl.CostEstimate(flops=a.size, bytes_accessed=4 * a.size, transcendentals=0),
        name="move",
    )(a)


def solution(mesh):
    def step(x, gain, wq, wk, wv, wo):
        return move(layer(Sizes(x.shape[0], x.shape[1], wq.shape[1] // HEAD), x, gain, wq, wk, wv, wo))

    tokens, columns = P("dp", None), P(None, "tp")
    return jax.shard_map(
        step,
        mesh=mesh,
        in_specs=(tokens, P(None), columns, columns, columns, P("tp", None)),
        out_specs=tokens,
        check_vma=False,
    )
```
